256 devices in a mesh: rows: 64 (over y, z, core), rhs: 4 (over x).
Axes of the slice: x: 4, y: 4, z: 8, core: 2. Of those that a mesh axis runs over, the one named last changes fastest.
Arguments:
- rhs: float32 [65536, 2048], P('rows', 'rhs'), parts along dimension 1, may hold values from -6 to 6
- leaf_inverse: float32 [65536, 1024], P('rows'), may hold values from -0.1875 to 0.1875
- basis_left: float32 [3, 65536, 128], P(None, 'rows'), may hold values from -0.5 to 0.5
- basis_right: float32 [3, 65536, 128], P(None, 'rows'), may hold values from -0.03125 to 0.03125
- cores: float32 [7, 256, 256], replicated, may hold values from -0.375 to 0.375
Outputs:
- solution: float32 [65536, 2048], P('rows', 'rhs'), parts along dimension 1
The draws below stay inside these ranges and needn't reach their ends.
There are 4 independent parts, one for each index of `rhs`. The reference program is written for one: setup_inputs(seed, part) draws one part's arguments, and reference() takes and returns one part's arrays. A program takes and returns all parts, laid end to end along the dimension named above; an argument that names none is the same for every part. Nothing has to cross between parts.
All inputs are finite; a program needn't handle non-finite values.
Results may differ from the reference program's by a relative error of at most 0.00011.
Values sent between devices are 32-bit elements; how exact they have to be, the bound alone decides.
No kernel may reach another device: no remote copies, remote signals or barrier semaphores. Data moves between devices by JAX's collectives and lax.ppermute only.
A program may use at most 64 MiB of HBM per device.

```python
import jax
import jax.numpy as jnp
from jax import lax

LEAF = 1024
R = 128
COLS = 512
LEVELS = 3
N = 65536
N_ROWS = 64


def shard_levels(stream_key, dims, shards, smallest, high):
    level, own = 1.0, jax.random.fold_in(stream_key, 6)
    for dim, parts in shards:
        heights = jnp.exp(jax.random.uniform(jax.random.fold_in(own, dim), (parts,), jnp.float32, smallest / len(shards), high / len(shards)))
        level = level * jnp.repeat(heights, dims[dim] // parts).reshape([-1 if axis == dim else 1 for axis in range(len(dims))])
    return level


def normal_values(own_key, dims, spread, most, split=(), held_as=jnp.bfloat16):
    array = spread * jax.random.normal(own_key, dims, jnp.float32)
    if split:
        array = array * shard_levels(own_key, dims, split, -0.22, 0.18)
    return jnp.clip(array, -most, most).astype(held_as)


def setup_inputs(seed: int = 0, part: int = 0) -> dict:
    seeds = jax.random.split(jax.random.key(seed), 6)
    part_keys = jax.random.split(jax.random.fold_in(seeds[5], part), 6)
    rhs = normal_values(part_keys[0], (N, COLS), 1.0, 6.0, ((0, 64),), jnp.float32)
    leaf_inverse = normal_values(seeds[1], (N, LEAF), LEAF ** -0.5, 0.1875, ((0, 64),), jnp.float32)
    basis_left = normal_values(seeds[2], (LEVELS, N, R), R ** -0.5, 0.5, ((1, 64),), jnp.float32)
    basis_right = normal_values(seeds[3], (LEVELS, N, R), (N // 2) ** -0.5, 0.03125, ((1, 64),), jnp.float32)
    cores = normal_values(seeds[4], (2 ** LEVELS - 1, 2 * R, 2 * R), (2 * R) ** -0.5, 0.375, (), jnp.float32)
    return {"rhs": rhs, "leaf_inverse": leaf_inverse, "basis_left": basis_left, "basis_right": basis_right, "cores": cores}


def reference(rhs, leaf_inverse, basis_left, basis_right, cores):
    highest = lax.Precision.HIGHEST
    total_rows = rhs.shape[0]
    columns = rhs.shape[1]
    leaves = leaf_inverse.reshape(N_ROWS, LEAF, LEAF)
    current = jnp.einsum('lij,ljc->lic', leaves, rhs.reshape(N_ROWS, LEAF, columns), precision=highest)
    current = current.reshape(total_rows, columns)
    for level_index in range(LEVELS, 0, -1):
        blocks = 2 ** level_index
        height = total_rows // blocks
        right_basis = basis_right[level_index - 1].reshape(blocks, height, R)
        left_basis = basis_left[level_index - 1].reshape(blocks, height, R)
        shaped = current.reshape(blocks, height, columns)
        partial_value = jnp.einsum('bnr,bnc->brc', right_basis, shaped, precision=highest)
        stacked = partial_value.reshape(blocks // 2, 2 * R, columns)
        core_block = cores[blocks // 2 - 1: blocks - 1]
        coefficients = jnp.einsum('jst,jtc->jsc', core_block, stacked, precision=highest).reshape(blocks, R, columns)
        shaped = shaped - jnp.einsum('bnr,brc->bnc', left_basis, coefficients, precision=highest)
        current = shaped.reshape(total_rows, columns)
    return current
```

```python
import jax
import jax.numpy as jnp
from jax import lax
from jax.sharding import PartitionSpec as P


ZS, YS, XS, CORES = 8, 4, 4, 2
RANK = 128


def dot(a, b, ca, cb):
    return lax.dot_general(
        a, b, (((ca,), (cb,)), ((), ())), precision=lax.Precision.HIGH, preferred_element_type=jnp.float32
    )


def swapped(x, mask, axis="rows"):
    size = lax.axis_size(axis)
    return lax.ppermute(x, axis, [(i, i ^ mask) for i in range(size)])


def absolute(parts, place):
    a = jnp.stack(parts)
    n = len(parts)
    bit = 1
    while bit < n:
        view = a.reshape((n // (2 * bit), 2, bit) + a.shape[1:])
        flipped = jnp.flip(view, 1).reshape(a.shape)
        a = jnp.where((place & bit) != 0, flipped, a)
        bit *= 2
    return a


def halves_swapped(a, flag, axes):
    for axis in axes:
        lo, hi = jnp.split(a, 2, axis)
        a = jnp.where(flag, jnp.concatenate([hi, lo], axis), a)
    return a


def on_device(rhs, leaf_inverse, basis_left, basis_right, cores):
    position = lax.axis_index("rows")
    x = lax.axis_index("rhs")
    core, z, y = position % 2, position // 2 % ZS, position // 16
    sib, parity, half = z // 4, y % 2, y // 2
    columns = rhs.shape[1]
    per_core = columns // CORES
    chunk = per_core // ZS

    g3 = dot(basis_left[2], basis_right[0:2], 0, 1).reshape(RANK, 2 * RANK)
    g2 = dot(basis_left[1], basis_right[0], 0, 0)
    gram = jnp.concatenate([g3, g2], axis=1)
    quarter = RANK // XS
    eighth = quarter // CORES
    gram = lax.dynamic_slice_in_dim(gram, x * quarter, quarter, 0).reshape(CORES, eighth, 3 * RANK)
    mine = lax.dynamic_index_in_dim(gram, core, 0, keepdims=False)
    other = lax.dynamic_index_in_dim(gram, 1 - core, 0, keepdims=False)
    mine = mine + swapped(other, 1)
    pieces = [mine] + [swapped(mine, 2 * m) for m in range(1, ZS)]
    own_sum = pieces[0] + pieces[1] + pieces[2] + pieces[3]
    oth_sum = pieces[4] + pieces[5] + pieces[6] + pieces[7]
    sums = jnp.stack([own_sum, oth_sum])
    pieces = [sums] + [swapped(sums, m, "rhs") for m in range(1, XS)]
    by_x = absolute(pieces, x)
    by_core = absolute([by_x, swapped(by_x, 1)], core)
    gram = by_core.transpose(2, 1, 0, 3, 4).reshape(2, RANK, 3 * RANK)
    gram3 = gram[:, :, : 2 * RANK].reshape(2 * RANK, 2 * RANK)
    gram2 = gram[0, :, 2 * RANK :] + gram[1, :, 2 * RANK :]
    gram2 = [gram2] + [swapped(gram2, 16 * m) for m in range(1, YS)]
    gram2_own = jnp.concatenate(gram2[:2], axis=0)
    gram2_oth = jnp.concatenate(gram2[2:], axis=0)

    core3 = halves_swapped(lax.dynamic_index_in_dim(cores, 3 + y, 0, keepdims=False), sib == 1, (0, 1))
    core2_own = halves_swapped(lax.dynamic_index_in_dim(cores, 1 + half, 0, keepdims=False), parity == 1, (0, 1))
    core2_oth = halves_swapped(lax.dynamic_index_in_dim(cores, 2 - half, 0, keepdims=False), parity == 1, (0, 1))
    core1 = halves_swapped(cores[0], half == 1, (0, 1))[:RANK]

    folded = dot(basis_right, leaf_inverse, 1, 0).reshape(3 * RANK, leaf_inverse.shape[1])
    q = dot(rhs, folded, 0, 1).reshape(CORES, per_core, 3 * RANK)
    mine = lax.dynamic_index_in_dim(q, core, 0, keepdims=False)
    other = lax.dynamic_index_in_dim(q, 1 - core, 0, keepdims=False)
    mine = mine + swapped(other, 1)
    pieces = [lax.dynamic_slice_in_dim(mine, (z ^ m) * chunk, chunk, 0) for m in range(ZS)]
    pieces = [pieces[0]] + [swapped(pieces[m], 2 * m) for m in range(1, ZS)]
    own = pieces[0] + pieces[1] + pieces[2] + pieces[3]
    oth = pieces[4] + pieces[5] + pieces[6] + pieces[7]

    p3 = jnp.concatenate([own[:, 2 * RANK :], oth[:, 2 * RANK :]], axis=1)
    c3 = dot(p3, core3, 1, 1)
    rest = own[:, : 2 * RANK] + oth[:, : 2 * RANK] - dot(c3, gram3, 1, 0)
    rests = [rest] + [swapped(rest, 16 * m) for m in range(1, YS)]
    p2 = [r[:, RANK:] for r in rests]
    c2_own = dot(jnp.concatenate(p2[:2], axis=1), core2_own, 1, 1)
    c2_oth = dot(jnp.concatenate(p2[2:], axis=1), core2_oth, 1, 1)
    p1_own = rests[0][:, :RANK] + rests[1][:, :RANK] - dot(c2_own, gram2_own, 1, 0)
    p1_oth = rests[2][:, :RANK] + rests[3][:, :RANK] - dot(c2_oth, gram2_oth, 1, 0)
    c1 = dot(jnp.concatenate([p1_own, p1_oth], axis=1), core1, 1, 1)
    to_own = jnp.concatenate([c1, c2_own[:, :RANK], c3[:, :RANK]], axis=1)
    to_oth = jnp.concatenate([c1, c2_own[:, :RANK], c3[:, RANK:]], axis=1)
    pieces = [to_own] + [swapped(to_own if m < 4 else to_oth, 2 * m) for m in range(1, ZS)]
    by_z = absolute(pieces, z).reshape(per_core, 3 * RANK)
    c = absolute([by_z, swapped(by_z, 1)], core).reshape(columns, 3 * RANK)

    y0 = dot(leaf_inverse, rhs, 1, 0)
    left = jnp.concatenate([basis_left[0], basis_left[1], basis_left[2]], axis=1)
    return y0 - dot(left, c, 1, 1)


def solution(mesh):
    placed = (P("rows", "rhs"), P("rows", None), P(None, "rows", None), P(None, "rows", None), P())
    return jax.shard_map(
        on_device, mesh=mesh, in_specs=placed, out_specs=P("rows", "rhs"), check_vma=False
    )
```

```python
import functools

import jax
import jax.numpy as jnp
from jax import lax
from jax.experimental import pallas as pl
from jax.experimental.pallas import tpu as pltpu
from jax.sharding import PartitionSpec as P


XS = 4
RANK = 128
LEAF = 1024
COLS = 512
QUARTER = RANK // XS
NN = (((1,), (0,)), ((), ()))
NT = (((1,), (1,)), ((), ()))
VMEM = pl.BlockSpec(memory_space=pltpu.VMEM)
SMEM = pl.BlockSpec(memory_space=pltpu.SMEM)
ANY = pl.BlockSpec(memory_space=pl.ANY)


def split(a):
    hi = a.astype(jnp.bfloat16)
    return hi, (a - hi.astype(jnp.float32)).astype(jnp.bfloat16)


def dot3(a, b, dims):
    ca, cb = dims[0][0][0], dims[0][1][0]
    lhs = jnp.concatenate([a[0], a[0], a[1]], axis=ca)
    rhs = jnp.concatenate([b[0], b[1], b[0]], axis=cb)
    return lax.dot_general(lhs, rhs, dims, preferred_element_type=jnp.float32)


def cost(flops, size):
    return pl.CostEstimate(flops=flops, bytes_accessed=size, transcendentals=0)


def params(mib):
    return pltpu.CompilerParams(vmem_limit_bytes=mib << 20)


def in_hbm(a):
    return pltpu.with_memory_space_constraint(a, pltpu.HBM)


def in_chip(*arrays):
    return tuple(pltpu.with_memory_space_constraint(a, pltpu.VMEM) for a in arrays)


def f32(*shape):
    return pltpu.VMEM(shape, jnp.float32)


def bf16(*shape):
    return pltpu.VMEM(shape, jnp.bfloat16)


def far(*shape):
    return pltpu.HBM(shape, jnp.float32)


def open_kernel(place, right, left2, left3, rhs, gram, x_hi, x_lo, acc):
    i = pl.program_id(0)

    @pl.when(i == 0)
    def _():
        acc[...] = jnp.zeros_like(acc)

    rows = pl.ds(pl.multiple_of(i * rhs.shape[0], rhs.shape[0]), rhs.shape[0])
    x_hi[rows, :], x_lo[rows, :] = split(rhs[...])
    rt = split(jnp.concatenate([right[0].T, right[1].T], axis=0))
    r1 = rt[0][:RANK], rt[1][:RANK]
    acc[:, : 2 * RANK] += dot3(split(left3[0].T), rt, NT)
    acc[:, 2 * RANK :] += dot3(split(left2[0].T), r1, NT)

    @pl.when(i == pl.num_programs(0) - 1)
    def _():
        gram[...] = acc[pl.ds(pl.multiple_of(place[0] * QUARTER, QUARTER), QUARTER), :]


def open_stage(place, right, left, rhs):
    steps = 2
    height = LEAF // steps
    return pl.pallas_call(
        open_kernel,
        grid=(steps,),
        in_specs=[
            SMEM,
            pl.BlockSpec((2, height, RANK), lambda i: (0, i, 0)),
            pl.BlockSpec((1, height, RANK), lambda i: (1, i, 0)),
            pl.BlockSpec((1, height, RANK), lambda i: (2, i, 0)),
            pl.BlockSpec((height, COLS), lambda i: (i, 0)),
        ],
        out_specs=[VMEM] * 3,
        out_shape=[f32(QUARTER, 3 * RANK), bf16(LEAF, COLS), bf16(LEAF, COLS)],
        scratch_shapes=[pltpu.VMEM((RANK, 3 * RANK), jnp.float32)],
        compiler_params=params(12),
        cost_estimate=cost(6 * LEAF * RANK * 3 * RANK, 4 << 20),
        name="open_stage",
    )(place, in_hbm(right), in_hbm(left), in_hbm(left), in_hbm(rhs))


def leaf_kernel(first, last, place, leaf, right, x_hi, x_lo, *rest):
    i = pl.program_id(0)
    y = dot3(split(leaf[...]), (x_hi[...], x_lo[...]), NN)
    rt = split(jnp.concatenate([right[0].T, right[1].T, right[2].T], axis=0))
    part = dot3(rt, split(y), NN)
    if first:
        y0, *ends = rest
    else:
        before, _, y0, *ends = rest
    acc = ends[-1]
    y0[...] = y

    @pl.when(i == 0)
    def _():
        acc[...] = part if first else before[...] + part

    @pl.when(i > 0)
    def _():
        acc[...] += part

    if not last:
        return
    keep, send = ends[:2]

    @pl.when(i == pl.num_programs(0) - 1)
    def _():
        q = acc[...]
        first_half, second_half = q[:, : COLS // 2].T, q[:, COLS // 2 :].T

        @pl.when(place[0] == 0)
        def _():
            keep[...] = first_half
            send[...] = second_half

        @pl.when(place[0] == 1)
        def _():
            keep[...] = second_half
            send[...] = first_half


def leaf_part(step, parts, place, leaf, right, halves, before=None, y0=None):
    first, last = step == 0, step == parts - 1
    steps = 2
    height = LEAF // parts // steps
    ends = [f32(COLS // 2, 3 * RANK)] * 2 if last else [f32(3 * RANK, COLS)]
    given = () if first else (*in_chip(before), in_hbm(y0))
    return pl.pallas_call(
        functools.partial(leaf_kernel, first, last),
        grid=(steps,),
        in_specs=[
            SMEM,
            pl.BlockSpec((height, LEAF), lambda i: (i + steps * step, 0)),
            pl.BlockSpec((3, height, RANK), lambda i: (0, i + steps * step, 0)),
            VMEM,
            VMEM,
        ]
        + ([] if first else [VMEM, ANY]),
        out_specs=[pl.BlockSpec((height, COLS), lambda i: (i + steps * step, 0))] + [VMEM] * len(ends),
        out_shape=[far(LEAF, COLS)] + ends,
        scratch_shapes=[pltpu.VMEM((3 * RANK, COLS), jnp.float32)] if last else [],
        input_output_aliases={} if first else {6: 0},
        compiler_params=params(16),
        cost_estimate=cost(6 * LEAF // parts * COLS * (LEAF + 3 * RANK), 2 << 20),
    )(place, in_hbm(leaf), in_hbm(right), *in_chip(*halves), *given)


def ready_kernel(place, left, core3, core2, core1, hi, lo, out3, out2, out1):
    for k in range(3):
        hi[:, k * RANK : (k + 1) * RANK], lo[:, k * RANK : (k + 1) * RANK] = split(left[k])

    @pl.when(pl.program_id(0) == 0)
    def _():
        out3[...], out2[...], out1[...] = core3[0], core2[0], core1[0]


def ready_stage(place, left, cores):
    steps = 4
    height = LEAF // steps
    node = (1, 2 * RANK, 2 * RANK)
    return pl.pallas_call(
        ready_kernel,
        grid_spec=pltpu.PrefetchScalarGridSpec(
            num_scalar_prefetch=1,
            grid=(steps,),
            in_specs=[
                pl.BlockSpec((3, height, RANK), lambda i, w: (0, i, 0)),
                pl.BlockSpec(node, lambda i, w: (w[0], 0, 0)),
                pl.BlockSpec(node, lambda i, w: (w[1], 0, 0)),
                pl.BlockSpec(node, lambda i, w: (0, 0, 0)),
            ],
            out_specs=[pl.BlockSpec((height, 3 * RANK), lambda i, w: (i, 0))] * 2
            + [pl.BlockSpec(node[1:], lambda i, w: (0, 0))] * 3,
        ),
        out_shape=[bf16(LEAF, 3 * RANK)] * 2 + [f32(*node[1:])] * 3,
        compiler_params=params(8),
        cost_estimate=cost(1 << 22, 3 << 20),
        name="ready_stage",
    )(place, in_hbm(left), in_hbm(cores), in_hbm(cores), in_hbm(cores))


def node3_kernel(place, own, oth, core, gram, c_own, rest):
    second = place[0] == 1
    a, b = own[...], oth[...]
    p_own, p_oth = a[:, 2 * RANK :], b[:, 2 * RANK :]
    p = jnp.concatenate([jnp.where(second, p_oth, p_own), jnp.where(second, p_own, p_oth)], axis=1)
    c = dot3(split(p), split(core[...]), NT)
    first_c, second_c = c[:, :RANK], c[:, RANK:]
    mine = jnp.where(second, second_c, first_c)
    other = jnp.where(second, first_c, second_c)
    c_own[...] = mine
    fix = dot3(split(jnp.concatenate([mine, other], axis=1)), split(gram[...]), NN)
    rest[...] = a[:, : 2 * RANK] + b[:, : 2 * RANK] - fix


def node2_kernel(place, own, oth, core, gram_own, gram_oth, c_own, rest):
    second = place[0] == 1
    a, b = own[...], oth[...]
    p_own, p_oth = a[:, RANK:], b[:, RANK:]
    p = jnp.concatenate([jnp.where(second, p_oth, p_own), jnp.where(second, p_own, p_oth)], axis=1)
    c = dot3(split(p), split(core[...]), NT)
    mine = jnp.where(second, c[:, RANK:], c[:, :RANK])
    other = jnp.where(second, c[:, :RANK], c[:, RANK:])
    c_own[...] = mine
    gram = jnp.concatenate([gram_own[...], gram_oth[...]], axis=0)
    fix = dot3(split(jnp.concatenate([mine, other], axis=1)), split(gram), NN)
    rest[...] = a[:, :RANK] + b[:, :RANK] - fix


def node1_kernel(place, own, oth, core, c2, c3, out):
    second = place[0] == 1
    a, b = own[...], oth[...]
    p = jnp.concatenate([jnp.where(second, b, a), jnp.where(second, a, b)], axis=1)
    c = dot3(split(p), split(core[...]), NT)
    mine = jnp.where(second, c[:, RANK:], c[:, :RANK])
    out[...] = jnp.concatenate([mine, c2[...], c3[...]], axis=1)


def in_vmem(kernel, shapes, place, *arrays):
    return pl.pallas_call(
        kernel,
        in_specs=[SMEM] + [VMEM] * len(arrays),
        out_specs=[VMEM] * len(shapes),
        out_shape=[f32(*shape) for shape in shapes],
        compiler_params=params(4),
        cost_estimate=cost(1 << 20, 1 << 18),
    )(place, *in_chip(*arrays))


def halves_kernel(place, a, b, send, keep):
    n = send.shape[0]
    own = pl.ds(pl.multiple_of(place[0] * n, n), n)
    oth = pl.ds(pl.multiple_of((1 - place[0]) * n, n), n)
    send[...] = a[oth, :] + b[oth, :]
    keep[...] = a[own, :] + b[own, :]


def halves(place, a, b):
    shape = (a.shape[0] // 2, a.shape[1])
    return in_vmem(halves_kernel, [shape, shape], place, a, b)


def add_kernel(place, a, b, out):
    out[...] = a[...] + b[...]


def add(place, a, b):
    return in_vmem(add_kernel, [a.shape], place, a, b)[0]


def beside_kernel(place, a, b, out):
    n = a.shape[1]
    out[:, :n] = a[...]
    out[:, n:] = b[...]


def ordered_kernel(place, mine, other, out):
    n = mine.shape[0]
    out[pl.ds(pl.multiple_of(place[0] * n, n), n), :] = mine[...]
    out[pl.ds(pl.multiple_of((1 - place[0]) * n, n), n), :] = other[...]


def ordered(place, mine, other):
    return in_vmem(ordered_kernel, [(2 * mine.shape[0], mine.shape[1])], place, mine, other)[0]


def grams_kernel(place, mine, other, gram3, gram2):
    n = mine.shape[0]
    for bit, part in ((place[0], mine), (1 - place[0], other)):
        start = pl.multiple_of(bit * n, n)
        gram3[pl.ds(start, n), :] = part[:, : 2 * RANK]
        gram3[pl.ds(start + RANK, n), :] = part[:, 3 * RANK : 5 * RANK]
        gram2[pl.ds(start, n), :] = part[:, 2 * RANK : 3 * RANK] + part[:, 5 * RANK :]


def correct_kernel(where, y0, l_hi, l_lo, c, *rest):
    out = rest[-1]
    n = y0.shape[0]
    rows = pl.ds(pl.multiple_of(pl.program_id(0) * n, n), n)
    out[...] = y0[...] - dot3((l_hi[rows, :], l_lo[rows, :]), split(c[...]), NT)


def correct(where, y0, left, c, into=None):
    steps = 2
    height = LEAF // steps
    given = () if into is None else (into,)
    return pl.pallas_call(
        correct_kernel,
        grid_spec=pltpu.PrefetchScalarGridSpec(
            num_scalar_prefetch=1,
            grid=(steps,),
            in_specs=[pl.BlockSpec((height, RANK), lambda i, w: (i, w[0]))] + [VMEM] * 3 + [ANY] * len(given),
            out_specs=pl.BlockSpec((height, RANK), lambda i, w: (i, w[0])),
        ),
        out_shape=far(LEAF, COLS),
        input_output_aliases={5: 0} if given else {},
        compiler_params=params(8),
        cost_estimate=cost(6 * LEAF * 3 * RANK * RANK, 1 << 20),
    )(where, in_hbm(y0), *in_chip(*left, c), *given)


def swapped(x, mask, axis="rows"):
    size = lax.axis_size(axis)
    return lax.ppermute(x, axis, [(i, i ^ mask) for i in range(size)])


def on_device(rhs, leaf_inverse, basis_left, basis_right, cores):
    position = lax.axis_index("rows").astype(jnp.int32)
    x = lax.axis_index("rhs").astype(jnp.int32)
    core, z, y = position & 1, (position >> 1) & 7, position >> 4
    sib, parity, half = z >> 2, y & 1, y >> 1
    low, high = (z & 1) ^ sib, ((z >> 1) & 1) ^ sib
    scalar = lambda v: v.reshape(1)

    gram, *rhs_halves = open_stage(scalar(x), basis_right, basis_left, rhs)
    parts = 2
    y0, *q = leaf_part(0, parts, scalar(core), leaf_inverse, basis_right, rhs_halves)
    for step in range(1, parts):
        y0, *q = leaf_part(step, parts, scalar(core), leaf_inverse, basis_right, rhs_halves, q[0], y0)
    keep, send = q
    got = swapped(send, 1)

    gram = add(scalar(x), gram, swapped(gram, 1))
    gram = add(scalar(x), gram, swapped(gram, 2))
    gram = add(scalar(x), gram, swapped(gram, 4))
    gram_sib = swapped(gram, 14)
    (sums,) = in_vmem(beside_kernel, [(QUARTER, 6 * RANK)], scalar(x), gram, gram_sib)
    sums = ordered(scalar(x & 1), sums, swapped(sums, 1, "rhs"))
    gram3, gram2 = in_vmem(
        grams_kernel,
        [(2 * RANK, 2 * RANK), (RANK, RANK)],
        scalar(x >> 1),
        sums,
        swapped(sums, 2, "rhs"),
    )
    gram2_oth = swapped(gram2, 16)

    send, keep = halves(scalar(low), keep, got)
    send, keep = halves(scalar(high), keep, swapped(send, 2))
    own = add(scalar(x), keep, swapped(send, 4))
    oth = swapped(own, 14)

    l_hi, l_lo, core3, core2, core1 = ready_stage(jnp.stack([3 + y, 1 + half]), basis_left, cores)

    chunk = (COLS // 8, RANK)
    c3, rest = in_vmem(
        node3_kernel, [chunk, (COLS // 8, 2 * RANK)], scalar(sib), own, oth, core3, gram3
    )
    rest_oth = swapped(rest, 16)
    c2, rest1 = in_vmem(
        node2_kernel, [chunk, chunk], scalar(parity), rest, rest_oth, core2, gram2, gram2_oth
    )
    rest1_oth = swapped(rest1, 32)
    (c,) = in_vmem(
        node1_kernel, [(COLS // 8, 3 * RANK)], scalar(half), rest1, rest1_oth, core1, c2, c3
    )
    c = ordered(scalar(high), c, swapped(c, 4))
    c_low = swapped(c, 2)
    c_core = swapped(c, 1)
    c_core_low = swapped(c_low, 1)

    left = l_hi, l_lo
    out = correct(scalar(2 * core + low), y0, left, c)
    out = correct(scalar(2 * (1 - core) + low), y0, left, c_core, out)
    out = correct(scalar(2 * core + 1 - low), y0, left, c_low, out)
    return correct(scalar(2 * (1 - core) + 1 - low), y0, left, c_core_low, out)


def solution(mesh):
    placed = (P("rows", "rhs"), P("rows", None), P(None, "rows", None), P(None, "rows", None), P())
    return jax.shard_map(
        on_device, mesh=mesh, in_specs=placed, out_specs=P("rows", "rhs"), check_vma=False
    )
```

```python
import jax
import jax.numpy as jnp
from jax import lax
from jax.experimental import pallas as pl
from jax.experimental.pallas import tpu as pltpu
from jax.sharding import PartitionSpec as P


XS = 4
RANK = 128
LEAF = 1024
COLS = 512
QUARTER = RANK // XS
EIGHTH = QUARTER // 2
BLOCKS = 128, 128, 256, 256, 256
NN = (((1,), (0,)), ((), ()))
NT = (((1,), (1,)), ((), ()))
VMEM = pl.BlockSpec(memory_space=pltpu.VMEM)
SMEM = pl.BlockSpec(memory_space=pltpu.SMEM)
ANY = pl.BlockSpec(memory_space=pl.ANY)
HBM = pl.BlockSpec(memory_space=pltpu.HBM)


def split(a):
    hi = a.astype(jnp.bfloat16)
    return hi, (a - hi.astype(jnp.float32)).astype(jnp.bfloat16)


def dot3(a, b, dims):
    ca, cb = dims[0][0][0], dims[0][1][0]
    lhs = jnp.concatenate([a[0], a[0], a[1]], axis=ca)
    rhs = jnp.concatenate([b[0], b[1], b[0]], axis=cb)
    return lax.dot_general(lhs, rhs, dims, preferred_element_type=jnp.float32)


def cost(flops, size):
    return pl.CostEstimate(flops=flops, bytes_accessed=size, transcendentals=0)


def params(mib):
    return pltpu.CompilerParams(vmem_limit_bytes=mib << 20)


def in_hbm(a):
    return pltpu.with_memory_space_constraint(a, pltpu.HBM)


def in_chip(*arrays):
    return tuple(pltpu.with_memory_space_constraint(a, pltpu.VMEM) for a in arrays)


def f32(*shape):
    return pltpu.VMEM(shape, jnp.float32)


def bf16(*shape):
    return pltpu.VMEM(shape, jnp.bfloat16)


def far(*shape):
    return pltpu.HBM(shape, jnp.float32)


def open_kernel(place, right, left2, left3, rhs, leaf, keep, send, x_hi, x_lo, ahead, acc, sem):
    i = pl.program_id(0)
    copy = pltpu.make_async_copy(leaf.at[: ahead.shape[0], :], ahead, sem)

    @pl.when(i == 0)
    def _():
        copy.start()
        acc[...] = jnp.zeros_like(acc)

    rows = pl.ds(pl.multiple_of(i * rhs.shape[0], rhs.shape[0]), rhs.shape[0])
    x_hi[rows, :], x_lo[rows, :] = split(rhs[...])
    rt = split(jnp.concatenate([right[0].T, right[1].T], axis=0))
    r1 = rt[0][:RANK], rt[1][:RANK]
    acc[:, : 2 * RANK] += dot3(split(left3[0].T), rt, NT)
    acc[:, 2 * RANK :] += dot3(split(left2[0].T), r1, NT)

    @pl.when(i == pl.num_programs(0) - 1)
    def _():
        start = place[0] * QUARTER
        keep[...] = acc[pl.ds(pl.multiple_of(start + place[1] * EIGHTH, EIGHTH), EIGHTH), :]
        send[...] = acc[pl.ds(pl.multiple_of(start + (1 - place[1]) * EIGHTH, EIGHTH), EIGHTH), :]
        copy.wait()


def open_stage(place, right, left, rhs, leaf):
    steps = 2
    height = LEAF // steps
    return pl.pallas_call(
        open_kernel,
        grid=(steps,),
        in_specs=[
            SMEM,
            pl.BlockSpec((2, height, RANK), lambda i: (0, i, 0)),
            pl.BlockSpec((1, height, RANK), lambda i: (1, i, 0)),
            pl.BlockSpec((1, height, RANK), lambda i: (2, i, 0)),
            pl.BlockSpec((height, COLS), lambda i: (i, 0)),
            HBM,
        ],
        out_specs=[VMEM] * 5,
        out_shape=[f32(EIGHTH, 3 * RANK)] * 2 + [bf16(LEAF, COLS), bf16(LEAF, COLS), f32(BLOCKS[0], LEAF)],
        scratch_shapes=[pltpu.VMEM((RANK, 3 * RANK), jnp.float32), pltpu.SemaphoreType.DMA],
        compiler_params=params(12),
        cost_estimate=cost(6 * LEAF * RANK * 3 * RANK, 4 << 20),
        name="open_stage",
    )(place, in_hbm(right), in_hbm(left), in_hbm(left), in_hbm(rhs), in_hbm(leaf))


def leaf_kernel(place, leaf, right, x_hi, x_lo, ahead, y0, keep, send, blocks, bases, y, acc, sems):
    count = len(BLOCKS)
    rows = [slice(sum(BLOCKS[:k]), sum(BLOCKS[: k + 1])) for k in range(count)]
    loads = [pltpu.make_async_copy(leaf.at[r, :], blocks.at[r, :], sems.at[k]) for k, r in enumerate(rows)]
    bases_load = pltpu.make_async_copy(right, bases, sems.at[0])
    stores = [pltpu.make_async_copy(y.at[r, :], y0.at[r, :], sems.at[count + k]) for k, r in enumerate(rows)]
    loads[1].start()
    bases_load.start()
    for load in loads[2:]:
        load.start()
    for k, here in enumerate(rows):
        if k:
            loads[k].wait()
        block = blocks[here, :] if k else ahead[...]
        part = dot3(split(block), (x_hi[...], x_lo[...]), NN)
        y[here, :] = part
        stores[k].start()
        if k == 0:
            bases_load.wait()
        rt = split(jnp.concatenate([bases[i, here, :].T for i in range(3)], axis=0))
        q = dot3(rt, split(part), NN)
        acc[...] = acc[...] + q if k else q
    first_half, second_half = acc[:, : COLS // 2].T, acc[:, COLS // 2 :].T

    @pl.when(place[0] == 0)
    def _():
        keep[...] = first_half
        send[...] = second_half

    @pl.when(place[0] == 1)
    def _():
        keep[...] = second_half
        send[...] = first_half

    for store in stores:
        store.wait()


def leaf_stage(place, leaf, right, *arrays):
    return pl.pallas_call(
        leaf_kernel,
        in_specs=[SMEM, HBM, HBM, VMEM, VMEM, VMEM],
        out_specs=[HBM, VMEM, VMEM],
        out_shape=[far(LEAF, COLS)] + [f32(COLS // 2, 3 * RANK)] * 2,
        scratch_shapes=[
            pltpu.VMEM((LEAF, LEAF), jnp.float32),
            pltpu.VMEM((3, LEAF, RANK), jnp.float32),
            pltpu.VMEM((LEAF, COLS), jnp.float32),
            pltpu.VMEM((3 * RANK, COLS), jnp.float32),
            pltpu.SemaphoreType.DMA((2 * len(BLOCKS),)),
        ],
        compiler_params=params(24),
        cost_estimate=cost(6 * LEAF * COLS * (LEAF + 3 * RANK), 8 << 20),
        name="leaf_stage",
    )(place, in_hbm(leaf), in_hbm(right), *in_chip(*arrays))


def ready_kernel(place, left, core3, core2, core1, hi, lo, out3, out2, out1):
    for k in range(3):
        hi[:, k * RANK : (k + 1) * RANK], lo[:, k * RANK : (k + 1) * RANK] = split(left[k])

    @pl.when(pl.program_id(0) == 0)
    def _():
        out3[...], out2[...], out1[...] = core3[0], core2[0], core1[0]


def ready_stage(place, left, cores):
    steps = 4
    height = LEAF // steps
    node = (1, 2 * RANK, 2 * RANK)
    return pl.pallas_call(
        ready_kernel,
        grid_spec=pltpu.PrefetchScalarGridSpec(
            num_scalar_prefetch=1,
            grid=(steps,),
            in_specs=[
                pl.BlockSpec((3, height, RANK), lambda i, w: (0, i, 0)),
                pl.BlockSpec(node, lambda i, w: (w[0], 0, 0)),
                pl.BlockSpec(node, lambda i, w: (w[1], 0, 0)),
                pl.BlockSpec(node, lambda i, w: (0, 0, 0)),
            ],
            out_specs=[pl.BlockSpec((height, 3 * RANK), lambda i, w: (i, 0))] * 2
            + [pl.BlockSpec(node[1:], lambda i, w: (0, 0))] * 3,
        ),
        out_shape=[bf16(LEAF, 3 * RANK)] * 2 + [f32(*node[1:])] * 3,
        compiler_params=params(8),
        cost_estimate=cost(1 << 22, 3 << 20),
        name="ready_stage",
    )(place, in_hbm(left), in_hbm(cores), in_hbm(cores), in_hbm(cores))


def node3_kernel(place, own, oth, core, gram, c_own, rest):
    second = place[0] == 1
    a, b = own[...], oth[...]
    p_own, p_oth = a[:, 2 * RANK :], b[:, 2 * RANK :]
    p = jnp.concatenate([jnp.where(second, p_oth, p_own), jnp.where(second, p_own, p_oth)], axis=1)
    c = dot3(split(p), split(core[...]), NT)
    first_c, second_c = c[:, :RANK], c[:, RANK:]
    mine = jnp.where(second, second_c, first_c)
    other = jnp.where(second, first_c, second_c)
    c_own[...] = mine
    fix = dot3(split(jnp.concatenate([mine, other], axis=1)), split(gram[...]), NN)
    rest[...] = a[:, : 2 * RANK] + b[:, : 2 * RANK] - fix


def node2_kernel(place, own, oth, core, gram_own, gram_oth, c_own, rest):
    second = place[0] == 1
    a, b = own[...], oth[...]
    p_own, p_oth = a[:, RANK:], b[:, RANK:]
    p = jnp.concatenate([jnp.where(second, p_oth, p_own), jnp.where(second, p_own, p_oth)], axis=1)
    c = dot3(split(p), split(core[...]), NT)
    mine = jnp.where(second, c[:, RANK:], c[:, :RANK])
    other = jnp.where(second, c[:, :RANK], c[:, RANK:])
    c_own[...] = mine
    gram = jnp.concatenate([gram_own[...], gram_oth[...]], axis=0)
    fix = dot3(split(jnp.concatenate([mine, other], axis=1)), split(gram), NN)
    rest[...] = a[:, :RANK] + b[:, :RANK] - fix


def node1_kernel(place, own, oth, core, c2, c3, out):
    second = place[0] == 1
    a, b = own[...], oth[...]
    p = jnp.concatenate([jnp.where(second, b, a), jnp.where(second, a, b)], axis=1)
    c = dot3(split(p), split(core[...]), NT)
    mine = jnp.where(second, c[:, RANK:], c[:, :RANK])
    out[...] = jnp.concatenate([mine, c2[...], c3[...]], axis=1)


def in_vmem(kernel, shapes, place, *arrays):
    return pl.pallas_call(
        kernel,
        in_specs=[SMEM] + [VMEM] * len(arrays),
        out_specs=[VMEM] * len(shapes),
        out_shape=[f32(*shape) for shape in shapes],
        compiler_params=params(4),
        cost_estimate=cost(1 << 20, 1 << 18),
    )(place, *in_chip(*arrays))


def halves_kernel(place, a, b, send, keep):
    n = send.shape[0]
    own = pl.ds(pl.multiple_of(place[0] * n, n), n)
    oth = pl.ds(pl.multiple_of((1 - place[0]) * n, n), n)
    send[...] = a[oth, :] + b[oth, :]
    keep[...] = a[own, :] + b[own, :]


def halves(place, a, b):
    shape = (a.shape[0] // 2, a.shape[1])
    return in_vmem(halves_kernel, [shape, shape], place, a, b)


def add_kernel(place, a, b, out):
    out[...] = a[...] + b[...]


def add(place, a, b):
    return in_vmem(add_kernel, [a.shape], place, a, b)[0]


def beside_kernel(place, a, b, out):
    n = 2 * RANK
    out[:, :n] = a[:, :n]
    out[:, n : 2 * n] = b[:, :n]
    out[:, 2 * n :] = a[:, n:] + b[:, n:]


def collect_kernel(place, *refs):
    out = refs[-1]
    for m, part in enumerate(refs[:-1]):
        out[pl.ds(pl.multiple_of((place[0] ^ m) * EIGHTH, EIGHTH), EIGHTH), :] = part[...]


def ordered_kernel(place, mine, other, out):
    n = mine.shape[0]
    out[pl.ds(pl.multiple_of(place[0] * n, n), n), :] = mine[...]
    out[pl.ds(pl.multiple_of((1 - place[0]) * n, n), n), :] = other[...]


def ordered(place, mine, other):
    return in_vmem(ordered_kernel, [(2 * mine.shape[0], mine.shape[1])], place, mine, other)[0]


def grams_kernel(place, mine, other, gram3, gram2):
    n = 2 * RANK
    for bit, part in ((place[0], mine), (1 - place[0], other)):
        for k in range(XS):
            here = slice(k * EIGHTH, (k + 1) * EIGHTH)
            start = pl.multiple_of(k * QUARTER + bit * EIGHTH, EIGHTH)
            gram3[pl.ds(start, EIGHTH), :] = part[here, :n]
            gram3[pl.ds(start + RANK, EIGHTH), :] = part[here, n : 2 * n]
            gram2[pl.ds(start, EIGHTH), :] = part[here, 2 * n :]


def early_kernel(where, y0, l_hi, l_lo, c, c_core, columns, out, ahead_a, ahead_b, sems):
    i = pl.program_id(0)
    copies = [
        pltpu.make_async_copy(y0.at[:, pl.ds(pl.multiple_of(where[2 + k] * RANK, RANK), RANK)], ahead, sems.at[k])
        for k, ahead in enumerate((ahead_a, ahead_b))
    ]

    @pl.when(i == 0)
    def _():
        for copy in copies:
            copy.start()

    half = out.shape[0]
    rows = pl.ds(pl.multiple_of(i % 2 * half, half), half)
    left = l_hi[rows, :], l_lo[rows, :]

    @pl.when(i < 2)
    def _():
        out[...] = columns[...] - dot3(left, split(c[...]), NT)

    @pl.when(i >= 2)
    def _():
        out[...] = columns[...] - dot3(left, split(c_core[...]), NT)

    @pl.when(i == pl.num_programs(0) - 1)
    def _():
        for copy in copies:
            copy.wait()


def late_kernel(where, l_hi, l_lo, c, columns, into, out):
    half = out.shape[0]
    rows = pl.ds(pl.multiple_of(pl.program_id(0) * half, half), half)
    out[...] = columns[rows, :] - dot3((l_hi[rows, :], l_lo[rows, :]), split(c[...]), NT)


def early_corrections(where, y0, left, c, c_core):
    block = pl.BlockSpec((LEAF // 2, RANK), lambda i, w: (i % 2, w[i // 2]))
    return pl.pallas_call(
        early_kernel,
        grid_spec=pltpu.PrefetchScalarGridSpec(
            num_scalar_prefetch=1,
            grid=(4,),
            in_specs=[HBM] + [VMEM] * 4 + [block],
            out_specs=[block, VMEM, VMEM],
            scratch_shapes=[pltpu.SemaphoreType.DMA((2,))],
        ),
        out_shape=[far(LEAF, COLS)] + [f32(LEAF, RANK)] * 2,
        compiler_params=params(8),
        cost_estimate=cost(12 * LEAF * 3 * RANK * RANK, 3 << 20),
        name="early",
    )(where, in_hbm(y0), *in_chip(*left, c, c_core), in_hbm(y0))


def late_correction(where, left, c, columns, into):
    block = pl.BlockSpec((LEAF // 2, RANK), lambda i, w: (i, w[0]))
    return pl.pallas_call(
        late_kernel,
        grid_spec=pltpu.PrefetchScalarGridSpec(
            num_scalar_prefetch=1,
            grid=(2,),
            in_specs=[VMEM] * 4 + [ANY],
            out_specs=block,
        ),
        out_shape=far(LEAF, COLS),
        input_output_aliases={5: 0},
        compiler_params=params(8),
        cost_estimate=cost(6 * LEAF * 3 * RANK * RANK, 1 << 20),
    )(where, *in_chip(*left, c, columns), into)


def swapped(x, mask, axis="rows"):
    size = lax.axis_size(axis)
    return lax.ppermute(x, axis, [(i, i ^ mask) for i in range(size)])


def on_device(rhs, leaf_inverse, basis_left, basis_right, cores):
    position = lax.axis_index("rows").astype(jnp.int32)
    x = lax.axis_index("rhs").astype(jnp.int32)
    core, z, y = position & 1, (position >> 1) & 7, position >> 4
    sib, parity, half = z >> 2, y & 1, y >> 1
    low, high = (z & 1) ^ sib, ((z >> 1) & 1) ^ sib
    scalar = lambda v: v.reshape(1)

    gram, gram_send, *arrays = open_stage(jnp.stack([x, core]), basis_right, basis_left, rhs, leaf_inverse)
    y0, keep, send = leaf_stage(scalar(core), leaf_inverse, basis_right, *arrays)
    got = swapped(send, 1)

    gram = add(scalar(x), gram, swapped(gram_send, 1))
    gram = add(scalar(x), gram, swapped(gram, 2))
    gram = add(scalar(x), gram, swapped(gram, 4))
    wide = (EIGHTH, 5 * RANK)
    (sums,) = in_vmem(beside_kernel, [wide], scalar(x), gram, swapped(gram, 14))
    sums = [sums] + [swapped(sums, m, "rhs") for m in range(1, XS)]
    (sums,) = in_vmem(collect_kernel, [(XS * wide[0], wide[1])], scalar(x), *sums)
    gram3, gram2 = in_vmem(grams_kernel, [(2 * RANK, 2 * RANK), (RANK, RANK)], scalar(core), sums, swapped(sums, 1))
    gram2_oth = swapped(gram2, 16)

    send, keep = halves(scalar(low), keep, got)
    send, keep = halves(scalar(high), keep, swapped(send, 2))
    own = add(scalar(x), keep, swapped(send, 4))
    oth = swapped(own, 14)

    l_hi, l_lo, core3, core2, core1 = ready_stage(jnp.stack([3 + y, 1 + half]), basis_left, cores)

    chunk = (COLS // 8, RANK)
    c3, rest = in_vmem(node3_kernel, [chunk, (COLS // 8, 2 * RANK)], scalar(sib), own, oth, core3, gram3)
    rest_oth = swapped(rest, 16)
    c2, rest1 = in_vmem(node2_kernel, [chunk, chunk], scalar(parity), rest, rest_oth, core2, gram2, gram2_oth)
    rest1_oth = swapped(rest1, 32)
    (c,) = in_vmem(node1_kernel, [(COLS // 8, 3 * RANK)], scalar(half), rest1, rest1_oth, core1, c2, c3)
    c = ordered(scalar(high), c, swapped(c, 4))
    c_low = swapped(c, 2)
    c_core = swapped(c, 1)
    c_core_low = swapped(c_low, 1)

    left = l_hi, l_lo
    order = jnp.stack([2 * core + low, 2 * (1 - core) + low, 2 * core + 1 - low, 2 * (1 - core) + 1 - low])
    out, ahead_a, ahead_b = early_corrections(order, y0, left, c, c_core)
    out = late_correction(order[2:3], left, c_low, ahead_a, out)
    return late_correction(order[3:4], left, c_core_low, ahead_b, out)


def solution(mesh):
    placed = (P("rows", "rhs"), P("rows", None), P(None, "rows", None), P(None, "rows", None), P())
    return jax.shard_map(on_device, mesh=mesh, in_specs=placed, out_specs=P("rows", "rhs"), check_vma=False)
```

```python
import jax
import jax.numpy as jnp
from jax import lax
from jax.experimental import pallas as pl
from jax.experimental.pallas import tpu as pltpu
from jax.sharding import PartitionSpec as P


XS = 4
RANK = 128
LEAF = 1024
COLS = 512
QUARTER = RANK // XS
EIGHTH = QUARTER // 2
BLOCKS = 64, 192, 256, 256, 256
BATCH = 256
NN = (((1,), (0,)), ((), ()))
NT = (((1,), (1,)), ((), ()))
VMEM = pl.BlockSpec(memory_space=pltpu.VMEM)
SMEM = pl.BlockSpec(memory_space=pltpu.SMEM)
ANY = pl.BlockSpec(memory_space=pl.ANY)
HBM = pl.BlockSpec(memory_space=pltpu.HBM)


def split(a):
    hi = a.astype(jnp.bfloat16)
    return hi, (a - hi.astype(jnp.float32)).astype(jnp.bfloat16)


def dot3(a, b, dims):
    ca, cb = dims[0][0][0], dims[0][1][0]
    lhs = jnp.concatenate([a[0], a[0], a[1]], axis=ca)
    rhs = jnp.concatenate([b[0], b[1], b[0]], axis=cb)
    return lax.dot_general(lhs, rhs, dims, preferred_element_type=jnp.float32)


def cost(flops, size):
    return pl.CostEstimate(flops=flops, bytes_accessed=size, transcendentals=0)


def params(mib):
    return pltpu.CompilerParams(vmem_limit_bytes=mib << 20)


def in_hbm(a):
    return pltpu.with_memory_space_constraint(a, pltpu.HBM)


def in_chip(*arrays):
    return tuple(pltpu.with_memory_space_constraint(a, pltpu.VMEM) for a in arrays)


def f32(*shape):
    return pltpu.VMEM(shape, jnp.float32)


def bf16(*shape):
    return pltpu.VMEM(shape, jnp.bfloat16)


def far(*shape):
    return pltpu.HBM(shape, jnp.float32)


def open_kernel(place, right, left2, left3, rhs, leaf, gram, x_hi, x_lo, ahead, acc, sem):
    i = pl.program_id(0)
    copy = pltpu.make_async_copy(leaf.at[: ahead.shape[0], :], ahead, sem)

    @pl.when(i == 0)
    def _():
        copy.start()
        acc[...] = jnp.zeros_like(acc)

    rows = pl.ds(pl.multiple_of(i * rhs.shape[0], rhs.shape[0]), rhs.shape[0])
    x_hi[rows, :], x_lo[rows, :] = split(rhs[...])
    rt = split(jnp.concatenate([right[0].T, right[1].T], axis=0))
    r1 = rt[0][:RANK], rt[1][:RANK]
    acc[:, : 2 * RANK] += dot3(split(left3[0].T), rt, NT)
    acc[:, 2 * RANK :] += dot3(split(left2[0].T), r1, NT)

    @pl.when(i == pl.num_programs(0) - 1)
    def _():
        gram[...] = acc[pl.ds(pl.multiple_of(place[0] * QUARTER, QUARTER), QUARTER), :]
        copy.wait()


def open_stage(place, right, left, rhs, leaf):
    steps = 2
    height = LEAF // steps
    return pl.pallas_call(
        open_kernel,
        grid=(steps,),
        in_specs=[
            SMEM,
            pl.BlockSpec((2, height, RANK), lambda i: (0, i, 0)),
            pl.BlockSpec((1, height, RANK), lambda i: (1, i, 0)),
            pl.BlockSpec((1, height, RANK), lambda i: (2, i, 0)),
            pl.BlockSpec((height, COLS), lambda i: (i, 0)),
            HBM,
        ],
        out_specs=[VMEM] * 4,
        out_shape=[f32(QUARTER, 3 * RANK), bf16(LEAF, COLS), bf16(LEAF, COLS), f32(BLOCKS[0], LEAF)],
        scratch_shapes=[pltpu.VMEM((RANK, 3 * RANK), jnp.float32), pltpu.SemaphoreType.DMA],
        compiler_params=params(12),
        cost_estimate=cost(6 * LEAF * RANK * 3 * RANK, 4 << 20),
        name="open_stage",
    )(place, in_hbm(right), in_hbm(left), in_hbm(left), in_hbm(rhs), in_hbm(leaf))


def leaf_kernel(place, leaf, right, x_hi, x_lo, ahead, y0, keep, send, blocks, bases, y, acc, sems):
    count = len(BLOCKS)
    rows = [slice(sum(BLOCKS[:k]), sum(BLOCKS[: k + 1])) for k in range(count)]
    loads = [pltpu.make_async_copy(leaf.at[r, :], blocks.at[r, :], sems.at[k]) for k, r in enumerate(rows)]
    bases_load = pltpu.make_async_copy(right, bases, sems.at[0])
    stores = [pltpu.make_async_copy(y.at[r, :], y0.at[r, :], sems.at[count + k]) for k, r in enumerate(rows)]
    loads[1].start()
    bases_load.start()
    for load in loads[2:]:
        load.start()
    projected = 0
    for k, here in enumerate(rows):
        if k:
            loads[k].wait()
        block = blocks[here, :] if k else ahead[...]
        y[here, :] = dot3(split(block), (x_hi[...], x_lo[...]), NN)
        stores[k].start()
        if k == 1:
            bases_load.wait()
        ready = here.stop if k == count - 1 else here.start // BATCH * BATCH
        while projected < ready:
            done = slice(projected, projected + BATCH)
            projected += BATCH
            rt = split(jnp.concatenate([bases[i, done, :].T for i in range(3)], axis=0))
            q = dot3(rt, split(y[done, :]), NN)
            acc[...] = acc[...] + q if done.start else q
    first_half, second_half = acc[:, : COLS // 2].T, acc[:, COLS // 2 :].T

    @pl.when(place[0] == 0)
    def _():
        keep[...] = first_half
        send[...] = second_half

    @pl.when(place[0] == 1)
    def _():
        keep[...] = second_half
        send[...] = first_half

    for store in stores:
        store.wait()


def leaf_stage(place, leaf, right, *arrays):
    return pl.pallas_call(
        leaf_kernel,
        in_specs=[SMEM, HBM, HBM, VMEM, VMEM, VMEM],
        out_specs=[HBM, VMEM, VMEM],
        out_shape=[far(LEAF, COLS)] + [f32(COLS // 2, 3 * RANK)] * 2,
        scratch_shapes=[
            pltpu.VMEM((LEAF, LEAF), jnp.float32),
            pltpu.VMEM((3, LEAF, RANK), jnp.float32),
            pltpu.VMEM((LEAF, COLS), jnp.float32),
            pltpu.VMEM((3 * RANK, COLS), jnp.float32),
            pltpu.SemaphoreType.DMA((2 * len(BLOCKS),)),
        ],
        compiler_params=params(24),
        cost_estimate=cost(6 * LEAF * COLS * (LEAF + 3 * RANK), 8 << 20),
        name="leaf_stage",
    )(place, in_hbm(leaf), in_hbm(right), *in_chip(*arrays))


def left_kernel(left, hi, lo):
    for k in range(3):
        hi[:, k * RANK : (k + 1) * RANK], lo[:, k * RANK : (k + 1) * RANK] = split(left[k])


def left_halves(left):
    steps = 4
    height = LEAF // steps
    return pl.pallas_call(
        left_kernel,
        grid=(steps,),
        in_specs=[pl.BlockSpec((3, height, RANK), lambda i: (0, i, 0))],
        out_specs=[pl.BlockSpec((height, 3 * RANK), lambda i: (i, 0))] * 2,
        out_shape=[bf16(LEAF, 3 * RANK)] * 2,
        compiler_params=params(8),
        cost_estimate=cost(1 << 22, 3 << 20),
        name="left_halves",
    )(in_hbm(left))


def pick_kernel(place, cores, out3, out2, out1, sems):
    copies = [
        pltpu.make_async_copy(cores.at[where], out, sems.at[k])
        for k, (where, out) in enumerate(((place[0], out3), (place[1], out2), (0, out1)))
    ]
    for copy in copies:
        copy.start()
    for copy in copies:
        copy.wait()


def pick_cores(place, cores):
    return pl.pallas_call(
        pick_kernel,
        in_specs=[SMEM, HBM],
        out_specs=[VMEM] * 3,
        out_shape=[f32(*cores.shape[1:])] * 3,
        scratch_shapes=[pltpu.SemaphoreType.DMA((3,))],
        compiler_params=params(4),
        cost_estimate=cost(1 << 20, 1 << 20),
        name="pick_cores",
    )(place, in_hbm(cores))


def node3_kernel(place, own, oth, core, gram, c_own, rest):
    second = place[0] == 1
    a, b = own[...], oth[...]
    p_own, p_oth = a[:, 2 * RANK :], b[:, 2 * RANK :]
    p = jnp.concatenate([jnp.where(second, p_oth, p_own), jnp.where(second, p_own, p_oth)], axis=1)
    c = dot3(split(p), split(core[...]), NT)
    first_c, second_c = c[:, :RANK], c[:, RANK:]
    mine = jnp.where(second, second_c, first_c)
    other = jnp.where(second, first_c, second_c)
    c_own[...] = mine
    fix = dot3(split(jnp.concatenate([mine, other], axis=1)), split(gram[...]), NN)
    rest[...] = a[:, : 2 * RANK] + b[:, : 2 * RANK] - fix


def node2_kernel(place, own, oth, core, gram_own, gram_oth, c_own, rest):
    second = place[0] == 1
    a, b = own[...], oth[...]
    p_own, p_oth = a[:, RANK:], b[:, RANK:]
    p = jnp.concatenate([jnp.where(second, p_oth, p_own), jnp.where(second, p_own, p_oth)], axis=1)
    c = dot3(split(p), split(core[...]), NT)
    mine = jnp.where(second, c[:, RANK:], c[:, :RANK])
    other = jnp.where(second, c[:, :RANK], c[:, RANK:])
    c_own[...] = mine
    gram = jnp.concatenate([gram_own[...], gram_oth[...]], axis=0)
    fix = dot3(split(jnp.concatenate([mine, other], axis=1)), split(gram), NN)
    rest[...] = a[:, :RANK] + b[:, :RANK] - fix


def node1_kernel(place, own, oth, core, c2, c3, out):
    second = place[0] == 1
    a, b = own[...], oth[...]
    p = jnp.concatenate([jnp.where(second, b, a), jnp.where(second, a, b)], axis=1)
    c = dot3(split(p), split(core[...]), NT)
    mine = jnp.where(second, c[:, RANK:], c[:, :RANK])
    out[...] = jnp.concatenate([mine, c2[...], c3[...]], axis=1)


def in_vmem(kernel, shapes, place, *arrays):
    return pl.pallas_call(
        kernel,
        in_specs=[SMEM] + [VMEM] * len(arrays),
        out_specs=[VMEM] * len(shapes),
        out_shape=[f32(*shape) for shape in shapes],
        compiler_params=params(4),
        cost_estimate=cost(1 << 20, 1 << 18),
    )(place, *in_chip(*arrays))


def halves_kernel(place, a, b, send, keep):
    n = send.shape[0]
    own = pl.ds(pl.multiple_of(place[0] * n, n), n)
    oth = pl.ds(pl.multiple_of((1 - place[0]) * n, n), n)
    send[...] = a[oth, :] + b[oth, :]
    keep[...] = a[own, :] + b[own, :]


def halves(place, a, b):
    shape = (a.shape[0] // 2, a.shape[1])
    return in_vmem(halves_kernel, [shape, shape], place, a, b)


def add_kernel(place, a, b, out):
    out[...] = a[...] + b[...]


def add(place, a, b):
    return in_vmem(add_kernel, [a.shape], place, a, b)[0]


def beside_kernel(place, a, b, out):
    n = 2 * RANK
    out[:, :n] = a[:, :n]
    out[:, n : 2 * n] = b[:, :n]
    out[:, 2 * n :] = a[:, n:] + b[:, n:]


def collect_kernel(place, *refs):
    out = refs[-1]
    for m, part in enumerate(refs[:-1]):
        out[pl.ds(pl.multiple_of((place[0] ^ m) * EIGHTH, EIGHTH), EIGHTH), :] = part[...]


def ordered_kernel(place, mine, other, out):
    n = mine.shape[0]
    out[pl.ds(pl.multiple_of(place[0] * n, n), n), :] = mine[...]
    out[pl.ds(pl.multiple_of((1 - place[0]) * n, n), n), :] = other[...]


def ordered(place, mine, other):
    return in_vmem(ordered_kernel, [(2 * mine.shape[0], mine.shape[1])], place, mine, other)[0]


def grams_kernel(place, mine, other, gram3, gram2):
    n = 2 * RANK
    for bit, part in ((place[0], mine), (1 - place[0], other)):
        for k in range(XS):
            here = slice(k * EIGHTH, (k + 1) * EIGHTH)
            start = pl.multiple_of(k * QUARTER + bit * EIGHTH, EIGHTH)
            gram3[pl.ds(start, EIGHTH), :] = part[here, :n]
            gram3[pl.ds(start + RANK, EIGHTH), :] = part[here, n : 2 * n]
            gram2[pl.ds(start, EIGHTH), :] = part[here, 2 * n :]


def early_kernel(where, y0, l_hi, l_lo, c, c_core, out, ahead_a, ahead_b, given, made, sems):
    def columns(ref, k):
        return ref.at[:, pl.ds(pl.multiple_of(where[k] * RANK, RANK), RANK)]

    targets = given.at[0], given.at[1], ahead_a, ahead_b
    loads = [pltpu.make_async_copy(columns(y0, k), target, sems.at[k]) for k, target in enumerate(targets)]
    stores = [pltpu.make_async_copy(made.at[k], columns(out, k), sems.at[4 + k]) for k in range(2)]
    for load in loads:
        load.start()
    for k, chunk in enumerate((c, c_core)):
        fix = dot3((l_hi[...], l_lo[...]), split(chunk[...]), NT)
        loads[k].wait()
        made[k] = given[k] - fix
        stores[k].start()
    for copy in loads[2:] + stores:
        copy.wait()


def late_kernel(where, l_hi, l_lo, c, columns, into, out):
    half = out.shape[0]
    rows = pl.ds(pl.multiple_of(pl.program_id(0) * half, half), half)
    out[...] = columns[rows, :] - dot3((l_hi[rows, :], l_lo[rows, :]), split(c[...]), NT)


def early_corrections(where, y0, left, c, c_core):
    return pl.pallas_call(
        early_kernel,
        in_specs=[SMEM, HBM] + [VMEM] * 4,
        out_specs=[HBM, VMEM, VMEM],
        out_shape=[far(LEAF, COLS)] + [f32(LEAF, RANK)] * 2,
        scratch_shapes=[pltpu.VMEM((2, LEAF, RANK), jnp.float32)] * 2 + [pltpu.SemaphoreType.DMA((6,))],
        compiler_params=params(12),
        cost_estimate=cost(12 * LEAF * 3 * RANK * RANK, 3 << 20),
        name="early",
    )(where, in_hbm(y0), *in_chip(*left, c, c_core))


def late_correction(where, left, c, columns, into):
    block = pl.BlockSpec((LEAF // 2, RANK), lambda i, w: (i, w[0]))
    return pl.pallas_call(
        late_kernel,
        grid_spec=pltpu.PrefetchScalarGridSpec(
            num_scalar_prefetch=1,
            grid=(2,),
            in_specs=[VMEM] * 4 + [ANY],
            out_specs=block,
        ),
        out_shape=far(LEAF, COLS),
        input_output_aliases={5: 0},
        compiler_params=params(8),
        cost_estimate=cost(6 * LEAF * 3 * RANK * RANK, 1 << 20),
    )(where, *in_chip(*left, c, columns), into)


def swapped(x, mask, axis="rows"):
    size = lax.axis_size(axis)
    return lax.ppermute(x, axis, [(i, i ^ mask) for i in range(size)])


def on_device(rhs, leaf_inverse, basis_left, basis_right, cores):
    position = lax.axis_index("rows").astype(jnp.int32)
    x = lax.axis_index("rhs").astype(jnp.int32)
    core, z, y = position & 1, (position >> 1) & 7, position >> 4
    sib, parity, half = z >> 2, y & 1, y >> 1
    low, high = (z & 1) ^ sib, ((z >> 1) & 1) ^ sib
    scalar = lambda v: v.reshape(1)

    gram, *arrays = open_stage(scalar(x), basis_right, basis_left, rhs, leaf_inverse)
    y0, keep, send = leaf_stage(scalar(core), leaf_inverse, basis_right, *arrays)
    got = swapped(send, 1)

    send_gram, gram = halves(scalar(core), gram, swapped(gram, 2))
    gram = add(scalar(x), gram, swapped(send_gram, 1))
    gram = add(scalar(x), gram, swapped(gram, 4))
    wide = (EIGHTH, 5 * RANK)
    (sums,) = in_vmem(beside_kernel, [wide], scalar(x), gram, swapped(gram, 14))
    sums = [sums] + [swapped(sums, m, "rhs") for m in range(1, XS)]
    (sums,) = in_vmem(collect_kernel, [(XS * wide[0], wide[1])], scalar(x), *sums)
    gram3, gram2 = in_vmem(grams_kernel, [(2 * RANK, 2 * RANK), (RANK, RANK)], scalar(core), sums, swapped(sums, 1))
    gram2_oth = swapped(gram2, 16)

    send, keep = halves(scalar(low), keep, got)
    send, keep = halves(scalar(high), keep, swapped(send, 2))
    own = add(scalar(x), keep, swapped(send, 4))
    oth = swapped(own, 14)

    core3, core2, core1 = pick_cores(jnp.stack([3 + y, 1 + half]), cores)

    chunk = (COLS // 8, RANK)
    c3, rest = in_vmem(node3_kernel, [chunk, (COLS // 8, 2 * RANK)], scalar(sib), own, oth, core3, gram3)
    rest_oth = swapped(rest, 16)
    c2, rest1 = in_vmem(node2_kernel, [chunk, chunk], scalar(parity), rest, rest_oth, core2, gram2, gram2_oth)
    rest1_oth = swapped(rest1, 32)
    (c,) = in_vmem(node1_kernel, [(COLS // 8, 3 * RANK)], scalar(half), rest1, rest1_oth, core1, c2, c3)
    c = ordered(scalar(high), c, swapped(c, 4))
    c_low = swapped(c, 2)
    c_core = swapped(c, 1)
    c_core_low = swapped(c_low, 1)

    left = left_halves(basis_left)
    order = jnp.stack([2 * core + low, 2 * (1 - core) + low, 2 * core + 1 - low, 2 * (1 - core) + 1 - low])
    out, ahead_a, ahead_b = early_corrections(order, y0, left, c, c_core)
    out = late_correction(order[2:3], left, c_low, ahead_a, out)
    return late_correction(order[3:4], left, c_core_low, ahead_b, out)


def solution(mesh):
    placed = (P("rows", "rhs"), P("rows", None), P(None, "rows", None), P(None, "rows", None), P())
    return jax.shard_map(on_device, mesh=mesh, in_specs=placed, out_specs=P("rows", "rhs"), check_vma=False)
```

```python
import jax
import jax.numpy as jnp
from jax import lax
from jax.experimental import pallas as pl
from jax.experimental.pallas import tpu as pltpu
from jax.sharding import PartitionSpec as P


XS = 4
RANK = 128
LEAF = 1024
COLS = 512
QUARTER = RANK // XS
EIGHTH = QUARTER // 2
BLOCKS = 64, 192, 256, 256, 256
BATCH = 256
NN = (((1,), (0,)), ((), ()))
NT = (((1,), (1,)), ((), ()))
VMEM = pl.BlockSpec(memory_space=pltpu.VMEM)
SMEM = pl.BlockSpec(memory_space=pltpu.SMEM)
ANY = pl.BlockSpec(memory_space=pl.ANY)
HBM = pl.BlockSpec(memory_space=pltpu.HBM)


def split(a):
    hi = a.astype(jnp.bfloat16)
    return hi, (a - hi.astype(jnp.float32)).astype(jnp.bfloat16)


def dot3(a, b, dims):
    ca, cb = dims[0][0][0], dims[0][1][0]
    lhs = jnp.concatenate([a[0], a[0], a[1]], axis=ca)
    rhs = jnp.concatenate([b[0], b[1], b[0]], axis=cb)
    return lax.dot_general(lhs, rhs, dims, preferred_element_type=jnp.float32)


def cost(flops, size):
    return pl.CostEstimate(flops=flops, bytes_accessed=size, transcendentals=0)


def params(mib):
    return pltpu.CompilerParams(vmem_limit_bytes=mib << 20)


def in_hbm(a):
    return pltpu.with_memory_space_constraint(a, pltpu.HBM)


def in_chip(*arrays):
    return tuple(pltpu.with_memory_space_constraint(a, pltpu.VMEM) for a in arrays)


def f32(*shape):
    return pltpu.VMEM(shape, jnp.float32)


def bf16(*shape):
    return pltpu.VMEM(shape, jnp.bfloat16)


def far(*shape):
    return pltpu.HBM(shape, jnp.float32)


def open_kernel(place, right, left2, left3, rhs, leaf, gram, x_hi, x_lo, ahead, acc, sem):
    i = pl.program_id(0)
    copy = pltpu.make_async_copy(leaf.at[: ahead.shape[0], :], ahead, sem)

    @pl.when(i == 0)
    def _():
        copy.start()
        acc[...] = jnp.zeros_like(acc)

    rows = pl.ds(pl.multiple_of(i * rhs.shape[0], rhs.shape[0]), rhs.shape[0])
    x_hi[rows, :], x_lo[rows, :] = split(rhs[...])
    rt = split(jnp.concatenate([right[0].T, right[1].T], axis=0))
    r1 = rt[0][:RANK], rt[1][:RANK]
    acc[:, : 2 * RANK] += dot3(split(left3[0].T), rt, NT)
    acc[:, 2 * RANK :] += dot3(split(left2[0].T), r1, NT)

    @pl.when(i == pl.num_programs(0) - 1)
    def _():
        gram[...] = acc[pl.ds(pl.multiple_of(place[0] * QUARTER, QUARTER), QUARTER), :]
        copy.wait()


def open_stage(place, right, left, rhs, leaf):
    steps = 2
    height = LEAF // steps
    return pl.pallas_call(
        open_kernel,
        grid=(steps,),
        in_specs=[
            SMEM,
            pl.BlockSpec((2, height, RANK), lambda i: (0, i, 0)),
            pl.BlockSpec((1, height, RANK), lambda i: (1, i, 0)),
            pl.BlockSpec((1, height, RANK), lambda i: (2, i, 0)),
            pl.BlockSpec((height, COLS), lambda i: (i, 0)),
            HBM,
        ],
        out_specs=[VMEM] * 4,
        out_shape=[f32(QUARTER, 3 * RANK), bf16(LEAF, COLS), bf16(LEAF, COLS), f32(BLOCKS[0], LEAF)],
        scratch_shapes=[pltpu.VMEM((RANK, 3 * RANK), jnp.float32), pltpu.SemaphoreType.DMA],
        compiler_params=params(12),
        cost_estimate=cost(6 * LEAF * RANK * 3 * RANK, 4 << 20),
        name="open_stage",
    )(place, in_hbm(right), in_hbm(left), in_hbm(left), in_hbm(rhs), in_hbm(leaf))


def leaf_kernel(place, leaf, right, x_hi, x_lo, ahead, y0, keep, send, blocks, bases, y, acc, sems):
    count = len(BLOCKS)
    rows = [slice(sum(BLOCKS[:k]), sum(BLOCKS[: k + 1])) for k in range(count)]
    loads = [pltpu.make_async_copy(leaf.at[r, :], blocks.at[r, :], sems.at[k]) for k, r in enumerate(rows)]
    bases_load = pltpu.make_async_copy(right, bases, sems.at[0])
    stores = [pltpu.make_async_copy(y.at[r, :], y0.at[r, :], sems.at[count + k]) for k, r in enumerate(rows)]
    loads[1].start()
    bases_load.start()
    for load in loads[2:]:
        load.start()
    projected = 0
    for k, here in enumerate(rows):
        if k:
            loads[k].wait()
        block = blocks[here, :] if k else ahead[...]
        y[here, :] = dot3(split(block), (x_hi[...], x_lo[...]), NN)
        stores[k].start()
        if k == 1:
            bases_load.wait()
        ready = here.stop if k == count - 1 else here.start // BATCH * BATCH
        while projected < ready:
            done = slice(projected, projected + BATCH)
            projected += BATCH
            rt = split(jnp.concatenate([bases[i, done, :].T for i in range(3)], axis=0))
            q = dot3(rt, split(y[done, :]), NN)
            acc[...] = acc[...] + q if done.start else q
    first_half, second_half = acc[:, : COLS // 2].T, acc[:, COLS // 2 :].T

    @pl.when(place[0] == 0)
    def _():
        keep[...] = first_half
        send[...] = second_half

    @pl.when(place[0] == 1)
    def _():
        keep[...] = second_half
        send[...] = first_half

    for store in stores:
        store.wait()


def leaf_stage(place, leaf, right, *arrays):
    return pl.pallas_call(
        leaf_kernel,
        in_specs=[SMEM, HBM, HBM, VMEM, VMEM, VMEM],
        out_specs=[HBM, VMEM, VMEM],
        out_shape=[far(LEAF, COLS)] + [f32(COLS // 2, 3 * RANK)] * 2,
        scratch_shapes=[
            pltpu.VMEM((LEAF, LEAF), jnp.float32),
            pltpu.VMEM((3, LEAF, RANK), jnp.float32),
            pltpu.VMEM((LEAF, COLS), jnp.float32),
            pltpu.VMEM((3 * RANK, COLS), jnp.float32),
            pltpu.SemaphoreType.DMA((2 * len(BLOCKS),)),
        ],
        compiler_params=params(24),
        cost_estimate=cost(6 * LEAF * COLS * (LEAF + 3 * RANK), 8 << 20),
        name="leaf_stage",
    )(place, in_hbm(leaf), in_hbm(right), *in_chip(*arrays))


def left_kernel(left, hi, lo):
    for k in range(3):
        hi[:, k * RANK : (k + 1) * RANK], lo[:, k * RANK : (k + 1) * RANK] = split(left[k])


def left_halves(left):
    steps = 4
    height = LEAF // steps
    return pl.pallas_call(
        left_kernel,
        grid=(steps,),
        in_specs=[pl.BlockSpec((3, height, RANK), lambda i: (0, i, 0))],
        out_specs=[pl.BlockSpec((height, 3 * RANK), lambda i: (i, 0))] * 2,
        out_shape=[bf16(LEAF, 3 * RANK)] * 2,
        compiler_params=params(8),
        cost_estimate=cost(1 << 22, 3 << 20),
        name="left_halves",
    )(in_hbm(left))


def pick_kernel(place, cores, out3, out2, out1, sems):
    copies = [
        pltpu.make_async_copy(cores.at[where], out, sems.at[k])
        for k, (where, out) in enumerate(((place[0], out3), (place[1], out2), (0, out1)))
    ]
    for copy in copies:
        copy.start()
    for copy in copies:
        copy.wait()


def pick_cores(place, cores):
    return pl.pallas_call(
        pick_kernel,
        in_specs=[SMEM, HBM],
        out_specs=[VMEM] * 3,
        out_shape=[f32(*cores.shape[1:])] * 3,
        scratch_shapes=[pltpu.SemaphoreType.DMA((3,))],
        compiler_params=params(4),
        cost_estimate=cost(1 << 20, 1 << 20),
        name="pick_cores",
    )(place, in_hbm(cores))


def node3_kernel(place, own, oth, core, gram, c_own, rest):
    second = place[0] == 1
    a, b = own[...], oth[...]
    p_own, p_oth = a[:, 2 * RANK :], b[:, 2 * RANK :]
    p = jnp.concatenate([jnp.where(second, p_oth, p_own), jnp.where(second, p_own, p_oth)], axis=1)
    c = dot3(split(p), split(core[...]), NT)
    first_c, second_c = c[:, :RANK], c[:, RANK:]
    mine = jnp.where(second, second_c, first_c)
    other = jnp.where(second, first_c, second_c)
    c_own[...] = mine
    fix = dot3(split(jnp.concatenate([mine, other], axis=1)), split(gram[...]), NN)
    rest[...] = a[:, : 2 * RANK] + b[:, : 2 * RANK] - fix


def node2_kernel(place, own, oth, core, gram_own, gram_oth, c_own, rest):
    second = place[0] == 1
    a, b = own[...], oth[...]
    p_own, p_oth = a[:, RANK:], b[:, RANK:]
    p = jnp.concatenate([jnp.where(second, p_oth, p_own), jnp.where(second, p_own, p_oth)], axis=1)
    c = dot3(split(p), split(core[...]), NT)
    mine = jnp.where(second, c[:, RANK:], c[:, :RANK])
    other = jnp.where(second, c[:, :RANK], c[:, RANK:])
    c_own[...] = mine
    gram = jnp.concatenate([gram_own[...], gram_oth[...]], axis=0)
    fix = dot3(split(jnp.concatenate([mine, other], axis=1)), split(gram), NN)
    rest[...] = a[:, :RANK] + b[:, :RANK] - fix


def node1_kernel(place, own, oth, core, c2, c3, out):
    second = place[0] == 1
    a, b = own[...], oth[...]
    p = jnp.concatenate([jnp.where(second, b, a), jnp.where(second, a, b)], axis=1)
    c = dot3(split(p), split(core[...]), NT)
    mine = jnp.where(second, c[:, RANK:], c[:, :RANK])
    out[...] = jnp.concatenate([mine, c2[...], c3[...]], axis=1)


def in_vmem(kernel, shapes, place, *arrays):
    return pl.pallas_call(
        kernel,
        in_specs=[SMEM] + [VMEM] * len(arrays),
        out_specs=[VMEM] * len(shapes),
        out_shape=[f32(*shape) for shape in shapes],
        compiler_params=params(4),
        cost_estimate=cost(1 << 20, 1 << 18),
    )(place, *in_chip(*arrays))


def halves_kernel(place, a, b, send, keep):
    n = send.shape[0]
    own = pl.ds(pl.multiple_of(place[0] * n, n), n)
    oth = pl.ds(pl.multiple_of((1 - place[0]) * n, n), n)
    send[...] = a[oth, :] + b[oth, :]
    keep[...] = a[own, :] + b[own, :]


def halves(place, a, b):
    shape = (a.shape[0] // 2, a.shape[1])
    return in_vmem(halves_kernel, [shape, shape], place, a, b)


def add_kernel(place, a, b, out):
    out[...] = a[...] + b[...]


def add(place, a, b):
    return in_vmem(add_kernel, [a.shape], place, a, b)[0]


def beside_kernel(place, a, b, out):
    n = 2 * RANK
    out[:, :n] = a[:, :n]
    out[:, n : 2 * n] = b[:, :n]
    out[:, 2 * n :] = a[:, n:] + b[:, n:]


def collect_kernel(place, *refs):
    out = refs[-1]
    for m, part in enumerate(refs[:-1]):
        out[pl.ds(pl.multiple_of((place[0] ^ m) * EIGHTH, EIGHTH), EIGHTH), :] = part[...]


def ordered_kernel(place, mine, other, out):
    n = mine.shape[0]
    out[pl.ds(pl.multiple_of(place[0] * n, n), n), :] = mine[...]
    out[pl.ds(pl.multiple_of((1 - place[0]) * n, n), n), :] = other[...]


def ordered(place, mine, other):
    return in_vmem(ordered_kernel, [(2 * mine.shape[0], mine.shape[1])], place, mine, other)[0]


def grams_kernel(place, mine, other, gram3, gram2):
    n = 2 * RANK
    for bit, part in ((place[0], mine), (1 - place[0], other)):
        for k in range(XS):
            here = slice(k * EIGHTH, (k + 1) * EIGHTH)
            start = pl.multiple_of(k * QUARTER + bit * EIGHTH, EIGHTH)
            gram3[pl.ds(start, EIGHTH), :] = part[here, :n]
            gram3[pl.ds(start + RANK, EIGHTH), :] = part[here, n : 2 * n]
            gram2[pl.ds(start, EIGHTH), :] = part[here, 2 * n :]


def early_kernel(where, y0, l_hi, l_lo, c, c_core, out, ahead_a, ahead_b, given, made, sems):
    def columns(ref, k):
        return ref.at[:, pl.ds(pl.multiple_of(where[k] * RANK, RANK), RANK)]

    targets = given.at[0], given.at[1], ahead_a, ahead_b
    loads = [pltpu.make_async_copy(columns(y0, k), target, sems.at[k]) for k, target in enumerate(targets)]
    for load in loads:
        load.start()
    both = split(jnp.concatenate([c[...], c_core[...]], axis=0))
    half = LEAF // 2
    stores = []
    for h in range(2):
        rows = slice(h * half, (h + 1) * half)
        fix = dot3((l_hi[rows, :], l_lo[rows, :]), both, NT)
        for k in range(2):
            if h == 0:
                loads[k].wait()
            made[k, rows, :] = given[k, rows, :] - fix[:, k * RANK : (k + 1) * RANK]
            start = pl.multiple_of(where[k] * RANK, RANK)
            store = pltpu.make_async_copy(
                made.at[k, rows, :], out.at[rows, pl.ds(start, RANK)], sems.at[4 + 2 * h + k]
            )
            store.start()
            stores.append(store)
    for copy in loads[2:] + stores:
        copy.wait()


def late_kernel(where, l_hi, l_lo, c, columns, into, out):
    half = out.shape[0]
    rows = pl.ds(pl.multiple_of(pl.program_id(0) * half, half), half)
    out[...] = columns[rows, :] - dot3((l_hi[rows, :], l_lo[rows, :]), split(c[...]), NT)


def early_corrections(where, y0, left, c, c_core):
    return pl.pallas_call(
        early_kernel,
        in_specs=[SMEM, HBM] + [VMEM] * 4,
        out_specs=[HBM, VMEM, VMEM],
        out_shape=[far(LEAF, COLS)] + [f32(LEAF, RANK)] * 2,
        scratch_shapes=[pltpu.VMEM((2, LEAF, RANK), jnp.float32)] * 2 + [pltpu.SemaphoreType.DMA((8,))],
        compiler_params=params(12),
        cost_estimate=cost(12 * LEAF * 3 * RANK * RANK, 3 << 20),
        name="early",
    )(where, in_hbm(y0), *in_chip(*left, c, c_core))


def late_correction(where, left, c, columns, into):
    block = pl.BlockSpec((LEAF // 2, RANK), lambda i, w: (i, w[0]))
    return pl.pallas_call(
        late_kernel,
        grid_spec=pltpu.PrefetchScalarGridSpec(
            num_scalar_prefetch=1,
            grid=(2,),
            in_specs=[VMEM] * 4 + [ANY],
            out_specs=block,
        ),
        out_shape=far(LEAF, COLS),
        input_output_aliases={5: 0},
        compiler_params=params(8),
        cost_estimate=cost(6 * LEAF * 3 * RANK * RANK, 1 << 20),
    )(where, *in_chip(*left, c, columns), into)


def swapped(x, mask, axis="rows"):
    size = lax.axis_size(axis)
    return lax.ppermute(x, axis, [(i, i ^ mask) for i in range(size)])


def on_device(rhs, leaf_inverse, basis_left, basis_right, cores):
    position = lax.axis_index("rows").astype(jnp.int32)
    x = lax.axis_index("rhs").astype(jnp.int32)
    core, z, y = position & 1, (position >> 1) & 7, position >> 4
    sib, parity, half = z >> 2, y & 1, y >> 1
    low, high = (z & 1) ^ sib, ((z >> 1) & 1) ^ sib
    scalar = lambda v: v.reshape(1)

    gram, *arrays = open_stage(scalar(x), basis_right, basis_left, rhs, leaf_inverse)
    y0, keep, send = leaf_stage(scalar(core), leaf_inverse, basis_right, *arrays)
    got = swapped(send, 1)

    send_gram, gram = halves(scalar(core), gram, swapped(gram, 2))
    gram = add(scalar(x), gram, swapped(send_gram, 1))
    gram = add(scalar(x), gram, swapped(gram, 4))
    wide = (EIGHTH, 5 * RANK)
    (sums,) = in_vmem(beside_kernel, [wide], scalar(x), gram, swapped(gram, 14))
    sums = [sums] + [swapped(sums, m, "rhs") for m in range(1, XS)]
    (sums,) = in_vmem(collect_kernel, [(XS * wide[0], wide[1])], scalar(x), *sums)
    gram3, gram2 = in_vmem(grams_kernel, [(2 * RANK, 2 * RANK), (RANK, RANK)], scalar(core), sums, swapped(sums, 1))
    gram2_oth = swapped(gram2, 16)

    send, keep = halves(scalar(low), keep, got)
    send, keep = halves(scalar(high), keep, swapped(send, 2))
    own = add(scalar(x), keep, swapped(send, 4))
    oth = swapped(own, 14)

    core3, core2, core1 = pick_cores(jnp.stack([3 + y, 1 + half]), cores)

    chunk = (COLS // 8, RANK)
    c3, rest = in_vmem(node3_kernel, [chunk, (COLS // 8, 2 * RANK)], scalar(sib), own, oth, core3, gram3)
    rest_oth = swapped(rest, 16)
    c2, rest1 = in_vmem(node2_kernel, [chunk, chunk], scalar(parity), rest, rest_oth, core2, gram2, gram2_oth)
    rest1_oth = swapped(rest1, 32)
    (c,) = in_vmem(node1_kernel, [(COLS // 8, 3 * RANK)], scalar(half), rest1, rest1_oth, core1, c2, c3)
    c = ordered(scalar(high), c, swapped(c, 4))
    c_low = swapped(c, 2)
    c_core = swapped(c, 1)
    c_core_low = swapped(c_low, 1)

    left = left_halves(basis_left)
    order = jnp.stack([2 * core + low, 2 * (1 - core) + low, 2 * core + 1 - low, 2 * (1 - core) + 1 - low])
    out, ahead_a, ahead_b = early_corrections(order, y0, left, c, c_core)
    out = late_correction(order[2:3], left, c_low, ahead_a, out)
    return late_correction(order[3:4], left, c_core_low, ahead_b, out)


def solution(mesh):
    placed = (P("rows", "rhs"), P("rows", None), P(None, "rows", None), P(None, "rows", None), P())
    return jax.shard_map(on_device, mesh=mesh, in_specs=placed, out_specs=P("rows", "rhs"), check_vma=False)
```
